256 devices in a mesh: grp: 2 (over y), ctx: 16 (over z), head: 4 (over x), sub: 2 (over core).
Axes of the slice: x: 4, y: 2, z: 16, core: 2. Of those that a mesh axis runs over, the one named last changes fastest.
The devices are a block of a 4x16x16 slice.
Arguments:
- hidden: bfloat16 [32768, 4096], P(('grp', 'ctx', 'sub')), parts along dimension 0, may hold values from -6 to 6
- query_hidden: bfloat16 [512, 4096], P(('grp', 'ctx', 'sub')), parts along dimension 0, may hold values from -6 to 6
- norm_gain: float32 [4096], replicated, may hold values from 0.1 to 1.9
- w_query: bfloat16 [4096, 2048], P(None, 'head'), may hold values from -8 to 8
- w_key: bfloat16 [4096, 512], P(None, 'head'), may hold values from -1 to 1
- w_value: bfloat16 [4096, 512], P(None, 'head'), may hold values from -0.09375 to 0.09375
Outputs:
- context_out: bfloat16 [32768, 2048], P(('grp', 'ctx', 'sub'), 'head'), parts along dimension 0
- query_out: bfloat16 [512, 2048], P(('grp', 'ctx', 'sub'), 'head'), parts along dimension 0
The draws below stay inside these ranges and needn't reach their ends.
There are 2 independent parts, one for each index of `grp`. The reference program is written for one: setup_inputs(seed, part) draws one part's arguments, and reference() takes and returns one part's arrays. A program takes and returns all parts, laid end to end along the dimension named above; an argument that names none is the same for every part. Nothing has to cross between parts.
All inputs are finite; a program needn't handle non-finite values.
Results may differ from the reference program's by a relative error of at most 0.018.
The reference program's roundings to bfloat16 on the way count: a program that leaves them out, or rounds other values in their place, can miss the bound.
Values may be sent and summed in bfloat16 or wider, within the bound.
No kernel may reach another device: no remote copies, remote signals or barrier semaphores. Data moves between devices by JAX's collectives and lax.ppermute only.
A program may use at most 64 MiB of HBM per device.

```python
import jax
import jax.numpy as jnp
from jax import lax

D = 4096
HEADS = 16
KV_HEADS = 4
HDIM = 128
CTX_DEV = 1024
Q_TOK = 256
CONTEXT = 16384
N_CTX = 16


def key_matrix(key):
    sample = jax.random.normal(jax.random.fold_in(key, 11), (D, KV_HEADS * HDIM), jnp.float32)
    return jnp.clip(sample, -6.0, 6.0) * D ** (-0.5)


def draw_w_key(key, part):
    return jnp.clip(key_matrix(key), -1.0, 1.0).astype(jnp.bfloat16)


def draw_w_query(key, part):
    noise_part = jnp.clip(jax.random.normal(jax.random.fold_in(key, 12), (D, HEADS * HDIM), jnp.float32), -6.0, 6.0) * D ** (-0.5)
    noise_part = 16.0 * noise_part
    return jnp.clip(noise_part, -8.0, 8.0).astype(jnp.bfloat16)


def shard_levels(own_key, extent, split, least, high):
    factor_of = 1.0
    for position, blocks in split:
        steps = jax.random.uniform(jax.random.fold_in(jax.random.fold_in(own_key, 6), position), (blocks,), jnp.float32, least / len(split), high / len(split))
        factor_of = factor_of * jnp.repeat(jnp.exp(steps), extent[position] // blocks).reshape((-1,) + (1,) * (len(extent) - 1 - position))
    return factor_of


def noise(stream_key, extent, width, bound, pieces=(), kind=jnp.bfloat16):
    loudness = shard_levels(stream_key, extent, pieces, -0.22, 0.18) if pieces else 1.0
    drawn = jax.random.normal(stream_key, extent, jnp.float32) * width * loudness
    return jnp.minimum(jnp.maximum(drawn, -bound), bound).astype(kind)


def setup_inputs(seed: int = 0, part: int = 0) -> dict:
    key_list = jax.random.split(jax.random.key(seed), 7)
    own_keys = jax.random.split(jax.random.fold_in(key_list[6], part), 7)
    return {
        "hidden": noise(own_keys[0], (CONTEXT, D), 1.0, 6.0, ((0, 32),)),
        "query_hidden": noise(own_keys[1], (Q_TOK, D), 1.0, 6.0, ((0, 32),)),
        "norm_gain": jnp.clip(1.0 + 0.18 * jax.random.normal(key_list[2], (D,), jnp.float32), 0.1, 1.9),
        "w_query": draw_w_query(jax.random.fold_in(key_list[6], 71), part),
        "w_key": draw_w_key(jax.random.fold_in(key_list[6], 71), part),
        "w_value": noise(key_list[5], (D, KV_HEADS * HDIM), D ** -0.5, 0.09375, ((1, 4),)),
    }


rope_base = 500000.0
norm_eps = 1e-05
masked_score = -1e+30

def normalize(states, norm_gain):
    widened = states.astype(jnp.float32)
    meansq = lax.optimization_barrier(jnp.mean(widened * widened, axis=-1, keepdims=True)) + norm_eps
    return (widened * lax.rsqrt(meansq) * norm_gain).astype(jnp.bfloat16)

def rotate(tensor, positions):
    half_dim = tensor.shape[-1] // 2
    inverse = rope_base ** (-(jnp.arange(half_dim, dtype=jnp.float32) * 2.0 / tensor.shape[-1]))
    angles = positions.astype(jnp.float32)[:, None] * inverse[None, :]
    cosine = jnp.cos(angles)[:, None, :]
    sine_part = jnp.sin(angles)[:, None, :]
    lower_half = tensor[..., :half_dim]
    upper_half = tensor[..., half_dim:]
    return jnp.concatenate([lower_half * cosine - upper_half * sine_part, upper_half * cosine + lower_half * sine_part], axis=-1)

def project(normed, positions, w_query, w_key, w_value):
    row_count = normed.shape[0]
    query_heads = jnp.dot(normed, w_query, preferred_element_type=jnp.float32).reshape(row_count, -1, HDIM)
    key_heads = jnp.dot(normed, w_key, preferred_element_type=jnp.float32).reshape(row_count, -1, HDIM)
    value_heads = jnp.dot(normed, w_value, preferred_element_type=jnp.float32).reshape(row_count, -1, HDIM)
    return (rotate(query_heads, positions).astype(jnp.bfloat16), rotate(key_heads, positions).astype(jnp.bfloat16), value_heads.astype(jnp.bfloat16))

def attend(query_heads, key_heads, value_heads, visible):
    row_count = query_heads.shape[0]
    head_count = query_heads.shape[1]
    kv_count = key_heads.shape[1]
    grouped = query_heads.reshape(row_count, kv_count, head_count // kv_count, HDIM)
    scores = jnp.einsum('nkgd,mkd->nkgm', grouped.astype(jnp.float32), key_heads.astype(jnp.float32)) * HDIM ** (-0.5)
    mask_full = visible[:, None, None, :]
    scores = jnp.where(mask_full, scores, masked_score)
    maxima = lax.optimization_barrier(jnp.max(scores, axis=-1))
    weights = jnp.where(mask_full, jnp.exp(scores - maxima[..., None]), 0.0)
    totals = lax.optimization_barrier(jnp.sum(weights, axis=-1))
    rounded = lax.optimization_barrier(weights.astype(jnp.bfloat16)).astype(jnp.float32)
    accumulated = jnp.einsum('nkgm,mkd->nkgd', rounded, value_heads.astype(jnp.float32))
    return (maxima.reshape(row_count, head_count), totals.reshape(row_count, head_count), accumulated.reshape(row_count, head_count, HDIM))

def reference(hidden, query_hidden, norm_gain, w_query, w_key, w_value):
    context_len = CTX_DEV * N_CTX
    positions = jnp.arange(context_len, dtype=jnp.int32)
    queries, key_rows, value_rows = project(normalize(hidden, norm_gain), positions, w_query, w_key, w_value)
    query_positions = context_len + jnp.arange(Q_TOK, dtype=jnp.int32)
    query_heads, query_keys, query_values = project(normalize(query_hidden, norm_gain), query_positions, w_query, w_key, w_value)
    anchor_keys = key_rows[:CTX_DEV]
    anchor_values = value_rows[:CTX_DEV]
    offsets = jnp.arange(CTX_DEV, dtype=jnp.int32)
    causal = offsets[:, None] >= offsets[None, :]

    def one_block(blocked):
        block_q, block_k, block_v, block_index = blocked
        all_keys = jnp.concatenate([anchor_keys, block_k], axis=0)
        all_values = jnp.concatenate([anchor_values, block_v], axis=0)
        visible = jnp.concatenate([jnp.broadcast_to(block_index > 0, (CTX_DEV, CTX_DEV)), causal], axis=1)
        maxima, totals, accumulated = attend(block_q, all_keys, all_values, visible)
        return (accumulated / totals[..., None]).astype(jnp.bfloat16).reshape(CTX_DEV, HEADS * HDIM)
    context_out = lax.map(one_block, (queries.reshape(N_CTX, CTX_DEV, HEADS, HDIM), key_rows.reshape(N_CTX, CTX_DEV, KV_HEADS, HDIM), value_rows.reshape(N_CTX, CTX_DEV, KV_HEADS, HDIM), jnp.arange(N_CTX, dtype=jnp.int32))).reshape(context_len, HEADS * HDIM)
    every_key = jnp.concatenate([key_rows, query_keys], axis=0)
    every_value = jnp.concatenate([value_rows, query_values], axis=0)
    block_rows = Q_TOK // N_CTX

    def one_rows(blocked):
        rows_q, rows_pos = blocked
        visible = jnp.concatenate([jnp.ones((block_rows, context_len), dtype=bool), rows_pos[:, None] >= query_positions[None, :]], axis=1)
        maxima, totals, accumulated = attend(rows_q, every_key, every_value, visible)
        return (accumulated / totals[..., None]).astype(jnp.bfloat16).reshape(block_rows, HEADS * HDIM)
    query_out = lax.map(one_rows, (query_heads.reshape(N_CTX, block_rows, HEADS, HDIM), query_positions.reshape(N_CTX, block_rows))).reshape(Q_TOK, HEADS * HDIM)
    return (context_out, query_out)
```

```python
import functools

import jax
import jax.numpy as jnp
import numpy as np
from jax import lax
from jax.experimental import pallas as pl
from jax.experimental.pallas import tpu as pltpu
from jax.sharding import PartitionSpec as P

HDIM = 128
HALF = HDIM // 2
rope_base = 500000.0
norm_eps = 1e-05
NEG = -1e30
UNIT = float(HDIM**-0.5 * np.log2(np.e))

F32 = jnp.float32
BF16 = jnp.bfloat16
PIECE = 40


def inverse_freqs():
    inv = rope_base ** (-(np.arange(HALF, dtype=np.float64) * 2.0 / HDIM))
    return np.concatenate([inv, inv])


def offset_tables(rows):
    angles = np.arange(rows, dtype=np.float64)[:, None] * inverse_freqs()[None, :]
    return np.cos(angles).astype(np.float32), np.sin(angles).astype(np.float32)


def position():
    ctx, sub = lax.axis_index("ctx"), lax.axis_index("sub")
    return ctx, sub, ctx * lax.axis_size("sub") + sub


def start_tables(slots, step, first):
    at = first + step * np.arange(slots, dtype=np.float64)
    angles = at[:, None] * inverse_freqs()[None, :]
    return np.concatenate([np.cos(angles), np.sin(angles)]).astype(np.float32)


def rope_at(tab, slot, cos_b, sin_b):
    slots = tab.shape[0] // 2
    cos_a, sin_a = tab[pl.ds(slot, 1), :], tab[pl.ds(slots + slot, 1), :]
    cos = cos_a * cos_b - sin_a * sin_b
    sin = sin_a * cos_b + cos_a * sin_b
    lane = lax.broadcasted_iota(jnp.int32, sin.shape, 1)
    return cos, jnp.where(lane < HALF, -sin, sin)


def rotate(x, cos, sin_signed):
    return x * cos + pltpu.roll(x, HALF, 1) * sin_signed


def normalized(x, gain):
    x = x.astype(F32)
    meansq = jnp.sum(x * x, axis=-1, keepdims=True) * (1.0 / x.shape[-1]) + norm_eps
    return (x * lax.rsqrt(meansq) * gain).astype(BF16)


def dot(a, b):
    return jnp.dot(a, b, preferred_element_type=F32)


def dot_t(a, b):
    return lax.dot_general(a, b, (((1,), (1,)), ((), ())), preferred_element_type=F32)


VM = pl.BlockSpec(memory_space=pltpu.VMEM)
ANYWHERE = pl.BlockSpec(memory_space=pltpu.HBM)


def near(x):
    return pltpu.with_memory_space_constraint(x, pltpu.VMEM)


def far_off(x):
    return pltpu.with_memory_space_constraint(x, pltpu.HBM)


def first_kernel(copies, qhid_h, gain_h, tabs_h, wq, qsend, qhid, gain, tabs, wqv, sems, small):
    chunks = sems.shape[0]
    depth = wq.shape[0] // chunks
    parts = [pl.ds(c * depth, depth) for c in range(chunks)]
    get = [pltpu.make_async_copy(wq.at[parts[c], :], wqv.at[parts[c], :], sems.at[c]) for c in range(chunks)]
    few = [
        pltpu.make_async_copy(qhid_h, qhid, small.at[0]),
        pltpu.make_async_copy(gain_h, gain, small.at[1]),
        pltpu.make_async_copy(tabs_h, tabs, small.at[2]),
    ]
    for copy in few + get:
        copy.start()
    for copy in few:
        copy.wait()
    _, _, slot = position()
    toks = qhid.shape[0]
    n = normalized(qhid[...], gain[...])
    cos8, sin8 = rope_at(tabs.at[2 * toks :, :], slot, tabs[:toks, :], tabs[toks : 2 * toks, :])
    total = None
    for c in range(chunks):
        get[c].wait()
        here = slice(c * depth, (c + 1) * depth)
        part = dot(n[:, here], wqv[here, :])
        total = part if total is None else total + part
    heads = total.shape[1] // HDIM
    piece = jnp.concatenate(
        [rotate(total[:, h * HDIM : (h + 1) * HDIM], cos8, sin8) for h in range(heads)], axis=0
    ).astype(BF16)
    for c in range(copies):
        qsend[c * piece.shape[0] : (c + 1) * piece.shape[0], :] = piece


def first_call(copies, slots, rows, qhid, gain, wq):
    toks, width = qhid.shape
    tabs = np.concatenate([*offset_tables(toks), start_tables(slots, toks, slots * rows)])
    heads = wq.shape[1] // HDIM
    return pl.pallas_call(
        functools.partial(first_kernel, copies),
        grid=(1,),
        in_specs=[ANYWHERE] * 4,
        out_specs=pl.BlockSpec((copies * toks * heads, HDIM), lambda i: (0, 0)),
        out_shape=jax.ShapeDtypeStruct((copies * toks * heads, HDIM), BF16),
        scratch_shapes=[
            pltpu.VMEM(qhid.shape, BF16),
            pltpu.VMEM(gain.shape, F32),
            pltpu.VMEM(tabs.shape, F32),
            pltpu.VMEM(wq.shape, BF16),
            pltpu.SemaphoreType.DMA((8,)),
            pltpu.SemaphoreType.DMA((3,)),
        ],
        cost_estimate=pl.CostEstimate(
            flops=2 * toks * width * heads * HDIM * 64, bytes_accessed=5 << 20, transcendentals=1 << 10
        ),
        name="first",
    )(far_off(qhid), far_off(gain), far_off(tabs), far_off(wq))


def project_rows(hid, gain, wk, wv, cosb, sinb, tab, slot, kv, n, x, wkv, sems, normed):
    tiles = x.shape[0]
    size = x.shape[1]
    get = [
        pltpu.make_async_copy(hid.at[pl.ds(t * size, size), :], x.at[t], sems.at[t]) for t in range(tiles)
    ]
    put = []
    for t in range(tiles):
        here = pl.ds(t * size, size)
        put.append(pltpu.make_async_copy(n.at[here, :], normed.at[here, :], sems.at[tiles + 2 + t]))
    get_k = pltpu.make_async_copy(wk, wkv.at[:, pl.ds(0, HDIM)], sems.at[tiles])
    get_v = pltpu.make_async_copy(wv, wkv.at[:, pl.ds(HDIM, HDIM)], sems.at[tiles + 1])
    get[0].start()
    get_k.start()
    get_v.start()
    for t in range(1, tiles):
        get[t].start()

    def finish(t):
        here = slice(t * size, (t + 1) * size)
        both = dot(n[here, :], wkv[...])
        cos, sin = rope_at(tab, slot, cosb[here, :], sinb[here, :])
        kv[here, :HDIM] = rotate(both[:, :HDIM], cos, sin).astype(BF16)
        kv[here, HDIM:] = both[:, HDIM:].astype(BF16)

    for t in range(tiles):
        get[t].wait()
        if t == 1:
            get_k.wait()
            get_v.wait()
        n[t * size : (t + 1) * size, :] = normalized(x[t], gain[...])
        put[t].start()
        if t:
            finish(t - 1)
    finish(tiles - 1)
    for copy in put:
        copy.wait()


def anchor_rows_kernel(gain, cosb, sinb, tab, hid, wk, wv, kv, normed, n, x, wkv, sems):
    ctx, _, slot = position()

    @pl.when(ctx == 0)
    def _():
        project_rows(hid, gain, wk, wv, cosb, sinb, tab, slot, kv, n, x, wkv, sems, normed)


def other_rows_kernel(
    qhid, gain, cosb, sinb, tab, qtab, kv0, hid, wk, wv, normed0, kv, normed, qkv, n, x, wkv, sems
):
    ctx, _, slot = position()
    toks = qhid.shape[0]
    del normed0

    @pl.when(ctx != 0)
    def _():
        project_rows(hid, gain, wk, wv, cosb, sinb, tab, slot, kv, n, x, wkv, sems, normed)

    @pl.when(ctx == 0)
    def _():
        get_k = pltpu.make_async_copy(wk, wkv.at[:, pl.ds(0, HDIM)], sems.at[0])
        get_v = pltpu.make_async_copy(wv, wkv.at[:, pl.ds(HDIM, HDIM)], sems.at[1])
        get_k.start()
        get_v.start()
        kv[...] = kv0[...]
        get_k.wait()
        get_v.wait()

    cos8, sin8 = rope_at(qtab, slot, cosb[:toks, :], sinb[:toks, :])
    both = dot(normalized(qhid[...], gain[...]), wkv[...])
    k8 = rotate(both[:, :HDIM], cos8, sin8)
    zero = jnp.zeros_like(k8)
    qkv[:, :HDIM] = jnp.concatenate([k8, zero], axis=0).astype(BF16)
    qkv[:, HDIM:] = jnp.concatenate([both[:, HDIM:], zero], axis=0).astype(BF16)


def rows_scratch(rows, width):
    tiles = 4
    return [
        pltpu.VMEM((tiles, rows // tiles, width), BF16),
        pltpu.VMEM((width, 2 * HDIM), BF16),
        pltpu.SemaphoreType.DMA((2 * tiles + 2,)),
    ]


def anchor_rows_call(slots, hid, gain, wk, wv):
    rows, width = hid.shape
    cosb, sinb = offset_tables(rows)
    tab = start_tables(slots, rows, 0)
    scratch = rows_scratch(rows, width)
    return pl.pallas_call(
        anchor_rows_kernel,
        in_specs=[VM] * 4 + [ANYWHERE] * 3,
        out_specs=[VM, ANYWHERE],
        out_shape=[pltpu.VMEM((rows, 2 * HDIM), BF16), pltpu.HBM((rows, width), BF16)],
        scratch_shapes=[pltpu.VMEM((rows, width), BF16)] + scratch,
        compiler_params=pltpu.CompilerParams(vmem_limit_bytes=24 << 20),
        cost_estimate=pl.CostEstimate(flops=1 << 20, bytes_accessed=1 << 20, transcendentals=rows),
        name="anchor_rows",
    )(gain, near(cosb), near(sinb), near(tab), far_off(hid), far_off(wk), far_off(wv))


def other_rows_call(slots, hid, qhid, gain, wk, wv, kv0, normed0):
    rows, width = hid.shape
    toks = qhid.shape[0]
    cosb, sinb = offset_tables(rows)
    qtab = start_tables(slots, toks, slots * rows)
    tab = start_tables(slots, rows, 0)
    return pl.pallas_call(
        other_rows_kernel,
        in_specs=[VM] * 7 + [ANYWHERE] * 4,
        input_output_aliases={10: 1},
        out_specs=[VM, ANYWHERE, VM],
        out_shape=[
            pltpu.VMEM((rows, 2 * HDIM), BF16),
            pltpu.HBM((rows, width), BF16),
            pltpu.VMEM((2 * toks, 2 * HDIM), BF16),
        ],
        scratch_shapes=[pltpu.VMEM((rows, width), BF16)] + rows_scratch(rows, width),
        compiler_params=pltpu.CompilerParams(vmem_limit_bytes=24 << 20),
        cost_estimate=pl.CostEstimate(
            flops=4 * rows * width * 2 * HDIM, bytes_accessed=6 << 20, transcendentals=rows
        ),
        name="kv_proj",
    )(qhid, gain, near(cosb), near(sinb), near(tab), qtab, near(kv0), far_off(hid), far_off(wk), far_off(wv), far_off(normed0))


def q_kernel(cosb, sinb, tab, normed, wq, q, nb, wb, acc, sems):
    _, _, slot = position()
    chunks = nb.shape[0]
    depth = wb.shape[1]
    half = normed.shape[0] // 2
    get = []
    for c in range(chunks):
        part = pl.ds(c * depth, depth)
        get.append(
            [
                pltpu.make_async_copy(wq.at[part, :], wb.at[c], sems.at[3 * c]),
                pltpu.make_async_copy(
                    normed.at[pl.ds(0, half), part], nb.at[c, pl.ds(0, half), :], sems.at[3 * c + 1]
                ),
                pltpu.make_async_copy(
                    normed.at[pl.ds(half, half), part], nb.at[c, pl.ds(half, half), :], sems.at[3 * c + 2]
                ),
            ]
        )
        for copy in get[c]:
            copy.start()
    for c in range(chunks):
        for copy in get[c]:
            copy.wait()
        part_sum = dot(nb[c], wb[c])
        if c == 0:
            acc[...] = part_sum
        elif c < chunks - 1:
            acc[...] += part_sum
        else:
            cos, sin = rope_at(tab, slot, cosb[...], sinb[...])
            for h in range(acc.shape[1] // HDIM):
                part = slice(h * HDIM, (h + 1) * HDIM)
                q[:, part] = rotate(acc[:, part] + part_sum[:, part], cos, sin).astype(BF16)


def q_call(slots, normed, wq):
    rows, width = normed.shape
    chunks = 4
    depth = width // chunks
    cosb, sinb = offset_tables(rows)
    tab = start_tables(slots, rows, 0)
    return pl.pallas_call(
        q_kernel,
        in_specs=[VM] * 3 + [ANYWHERE] * 2,
        out_specs=VM,
        out_shape=pltpu.VMEM((rows, wq.shape[1]), BF16),
        scratch_shapes=[
            pltpu.VMEM((chunks, rows, depth), BF16),
            pltpu.VMEM((chunks, depth, wq.shape[1]), BF16),
            pltpu.VMEM((rows, wq.shape[1]), F32),
            pltpu.SemaphoreType.DMA((3 * chunks,)),
        ],
        compiler_params=pltpu.CompilerParams(vmem_limit_bytes=24 << 20),
        cost_estimate=pl.CostEstimate(
            flops=2 * rows * width * wq.shape[1], bytes_accessed=8 << 20, transcendentals=rows
        ),
        name="q_proj",
    )(near(cosb), near(sinb), near(tab), far_off(normed), far_off(wq))


def three(x):
    a = x.astype(BF16).astype(F32)
    b = (x - a).astype(BF16).astype(F32)
    return a, b, x - a - b


def partial_kernel(toks, q, kva, kvb, qkva, qkvb, out):
    steps = 4
    rows = q.shape[0] // steps
    group = out.shape[0] // PIECE // steps

    def body(i, carry):
        here = pl.ds(pl.multiple_of(i * rows, rows), rows)
        there = pl.ds(pl.multiple_of(i * group * PIECE, 16), group * PIECE)
        partial_rows(toks, i * group, q[here, :], kva, kvb, qkva, qkvb, out.at[there, :])
        return carry

    lax.fori_loop(0, steps, body, 0)


def partial_rows(toks, first, qv, kva, kvb, qkva, qkvb, out):
    rows = qv.shape[0]
    group = out.shape[0] // PIECE
    per = rows // group
    ctx, sub, _ = position()
    kq = jnp.concatenate([qkva[:, :HDIM], qkvb[:, :HDIM]], axis=0)
    vq = jnp.concatenate([qkva[:, HDIM:], qkvb[:, HDIM:]], axis=0)
    pad = jnp.zeros((HDIM - kq.shape[0], HDIM), BF16)
    kq = jnp.concatenate([kq, pad], axis=0)
    vq = jnp.concatenate([vq, pad], axis=0)
    sa = dot_t(qv, kva[:, :HDIM])
    sb = dot_t(qv, kvb[:, :HDIM])
    sq = dot_t(qv, kq)
    row = lax.broadcasted_iota(jnp.int32, sq.shape, 0)
    col = lax.broadcasted_iota(jnp.int32, sq.shape, 1)
    slot = (first + row // per) * 2 + sub
    token = slot * toks + row % toks
    sibling = (col >= 2 * toks).astype(jnp.int32)
    key_sub = jnp.where(sibling == 1, 1 - sub, sub)
    key_pos = col - sibling * (2 * toks)
    key_token = (ctx * 2 + key_sub) * toks + key_pos
    seen = (key_pos < toks) & (token >= key_token)
    sq = jnp.where(seen, sq, NEG)
    m = jnp.maximum(
        jnp.max(jnp.maximum(sa, sb), axis=1, keepdims=True), jnp.max(sq, axis=1, keepdims=True)
    )
    mu = m * UNIT
    pa = jnp.exp2(sa * UNIT - mu)
    pb = jnp.exp2(sb * UNIT - mu)
    pq = jnp.where(seen, jnp.exp2(sq * UNIT - mu), 0.0)
    s = jnp.sum(pa + pb, axis=1, keepdims=True) + jnp.sum(pq, axis=1, keepdims=True)
    acc = (
        dot(pa.astype(BF16), kva[:, HDIM:])
        + dot(pb.astype(BF16), kvb[:, HDIM:])
        + dot(pq.astype(BF16), vq)
    )
    lane = lax.broadcasted_iota(jnp.int32, acc.shape, 1)
    kind = lane % 8
    packed = jnp.zeros_like(acc)
    for n, value in enumerate(three(mu) + three(s)):
        packed = jnp.where(kind == n, value, packed)
    packed = jnp.where(lane // 8 == row % 16, packed, 0.0)
    for g in range(group):
        base = g * PIECE
        out[base : base + per, :] = acc[g * per : (g + 1) * per, :].astype(BF16)
        low = jnp.sum(packed[g * per : g * per + 16, :], axis=0, keepdims=True)
        high = jnp.sum(packed[g * per + 16 : (g + 1) * per, :], axis=0, keepdims=True)
        eight = lax.broadcasted_iota(jnp.int32, (8, HDIM), 0)
        out[base + per : base + PIECE, :] = jnp.where(eight == 0, low, high).astype(BF16)


def partial_call(toks, q, kva, kvb, qkva, qkvb):
    rows = q.shape[0]
    return pl.pallas_call(
        functools.partial(partial_kernel, toks),
        in_specs=[VM] * 5,
        out_specs=VM,
        out_shape=pltpu.VMEM((rows // 32 * PIECE, HDIM), BF16),
        compiler_params=pltpu.CompilerParams(vmem_limit_bytes=24 << 20),
        cost_estimate=pl.CostEstimate(
            flops=4 * rows * 2 * kva.shape[0] * HDIM,
            bytes_accessed=1 << 20,
            transcendentals=rows * 2 * kva.shape[0],
        ),
        name="query_partial",
    )(near(q), near(kva), near(kvb), near(qkva), near(qkvb))


def mark_kernel(anything, out):
    out[...] = anything[:8, :HDIM].astype(F32)


def mark_call(anything):
    return pl.pallas_call(
        mark_kernel,
        in_specs=[VM],
        out_specs=VM,
        out_shape=pltpu.VMEM((8, HDIM), F32),
        compiler_params=pltpu.CompilerParams(vmem_limit_bytes=4 << 20),
        cost_estimate=pl.CostEstimate(flops=1 << 10, bytes_accessed=1 << 12, transcendentals=0),
        name="mark",
    )(near(anything))


def combine_kernel(peers, parts, mark, out):
    del mark
    per = 32
    lane = lax.broadcasted_iota(jnp.int32, (per, HDIM), 1)
    row = lax.broadcasted_iota(jnp.int32, (per, HDIM), 0)
    mine = lane // 8 == row % 16
    spread = []
    for p in range(peers):
        block = parts[p * PIECE + per : (p + 1) * PIECE, :].astype(F32)
        spread.append(jnp.where(mine, jnp.where(row < 16, block[0:1, :], block[1:2, :]), 0.0))
    spread = jnp.concatenate(spread, axis=0).astype(BF16)
    kind = lax.broadcasted_iota(jnp.int32, (HDIM, HDIM), 0) % 8
    of_max = jnp.where(kind < 3, 1.0, 0.0)
    of_sum = jnp.where((kind >= 3) & (kind < 6), 1.0, 0.0)
    stats = dot(spread, jnp.concatenate([of_max, of_sum], axis=1).astype(BF16))
    ms = [stats[p * per : (p + 1) * per, :HDIM] for p in range(peers)]
    top = functools.reduce(jnp.maximum, ms)
    total = jnp.zeros_like(top)
    acc = jnp.zeros_like(top)
    for p in range(peers):
        factor = jnp.exp2(ms[p] - top)
        total += stats[p * per : (p + 1) * per, HDIM:] * factor
        acc += parts[p * PIECE : p * PIECE + per, :].astype(F32) * factor
    res = acc / total
    toks = out.shape[0]
    for h in range(per // toks):
        out[:, h * HDIM : (h + 1) * HDIM] = res[h * toks : (h + 1) * toks, :].astype(BF16)


def combine_call(peers, toks, parts, mark):
    return pl.pallas_call(
        functools.partial(combine_kernel, peers),
        in_specs=[VM] * 2,
        out_specs=VM,
        compiler_params=pltpu.CompilerParams(vmem_limit_bytes=16 << 20),
        out_shape=jax.ShapeDtypeStruct((toks, 32 // toks * HDIM), BF16),
        cost_estimate=pl.CostEstimate(flops=1 << 20, bytes_accessed=1 << 18, transcendentals=1 << 12),
        name="query_combine",
    )(near(parts), near(mark))


def own_kernel(q, kva, kvb, acc, stat):
    _, sub, _ = position()
    rows = q.shape[0]
    tile = 256
    heads = q.shape[1] // HDIM

    def run(second):
        for t in range(rows // tile):
            here = slice(t * tile, (t + 1) * tile)
            upto = (t + 1) * tile
            lane = lax.broadcasted_iota(jnp.int32, (tile, HDIM), 1)
            packed = jnp.zeros((tile, HDIM), F32)
            for h in range(heads):
                part = slice(h * HDIM, (h + 1) * HDIM)
                qv = q[here, part]
                so = dot_t(qv, kva[:upto, :HDIM])
                row = lax.broadcasted_iota(jnp.int32, so.shape, 0) + t * tile
                col = lax.broadcasted_iota(jnp.int32, so.shape, 1)
                so = jnp.where(col <= row, so, NEG)
                m = jnp.max(so, axis=1, keepdims=True)
                if second:
                    sb = dot_t(qv, kvb[:, :HDIM])
                    m = jnp.maximum(m, jnp.max(sb, axis=1, keepdims=True))
                mu = m * UNIT
                po = jnp.exp2(so * UNIT - mu)
                s = jnp.sum(po, axis=1, keepdims=True)
                a = dot(po.astype(BF16), kva[:upto, HDIM:])
                if second:
                    pb = jnp.exp2(sb * UNIT - mu)
                    s = s + jnp.sum(pb, axis=1, keepdims=True)
                    a = a + dot(pb.astype(BF16), kvb[:, HDIM:])
                acc[here, part] = a
                packed = jnp.where(lane == h, mu, packed)
                packed = jnp.where(lane == heads + h, s, packed)
            stat[here, :] = packed

    @pl.when(sub == 0)
    def _():
        run(False)

    @pl.when(sub != 0)
    def _():
        run(True)


def own_call(q, kva, kvb):
    rows = q.shape[0]
    return pl.pallas_call(
        own_kernel,
        in_specs=[VM] * 3,
        out_specs=[VM] * 2,
        out_shape=[pltpu.VMEM(q.shape, F32), pltpu.VMEM((rows, HDIM), F32)],
        compiler_params=pltpu.CompilerParams(vmem_limit_bytes=24 << 20),
        cost_estimate=pl.CostEstimate(
            flops=4 * rows * 4 * 2 * rows * HDIM, bytes_accessed=3 << 20, transcendentals=4 * rows * 2 * rows
        ),
        name="own_block",
    )(near(q), near(kva), near(kvb))


def anchor_kernel(q, kva, kvb, acc, stat, out):
    ctx, _, _ = position()
    heads = q.shape[1] // HDIM
    size = 256

    def column(here, n):
        lane = lax.broadcasted_iota(jnp.int32, (size, HDIM), 1)
        return jnp.sum(jnp.where(lane == n, stat[here, :], 0.0), axis=1, keepdims=True)

    def plain(i, carry):
        here = pl.ds(pl.multiple_of(i * size, size), size)
        for h in range(heads):
            part = slice(h * HDIM, (h + 1) * HDIM)
            out[here, part] = (acc[here, part] / column(here, heads + h)).astype(BF16)
        return carry

    def joined(i, carry):
        here = pl.ds(pl.multiple_of(i * size, size), size)
        for h in range(heads):
            part = slice(h * HDIM, (h + 1) * HDIM)
            qv = q[here, part]
            sa = dot_t(qv, kva[:, :HDIM])
            sb = dot_t(qv, kvb[:, :HDIM])
            m = jnp.max(jnp.maximum(sa, sb), axis=1, keepdims=True)
            before = column(here, h)
            mu = jnp.maximum(m * UNIT, before)
            pa = jnp.exp2(sa * UNIT - mu)
            pb = jnp.exp2(sb * UNIT - mu)
            factor = jnp.exp2(before - mu)
            s = column(here, heads + h) * factor + jnp.sum(pa + pb, axis=1, keepdims=True)
            a = (
                acc[here, part] * factor
                + dot(pa.astype(BF16), kva[:, HDIM:])
                + dot(pb.astype(BF16), kvb[:, HDIM:])
            )
            out[here, part] = (a / s).astype(BF16)
        return carry

    @pl.when(ctx == 0)
    def _():
        lax.fori_loop(0, q.shape[0] // size, plain, 0)

    @pl.when(ctx != 0)
    def _():
        lax.fori_loop(0, q.shape[0] // size, joined, 0)


def anchor_call(q, kva, kvb, acc, stat):
    rows = q.shape[0]
    return pl.pallas_call(
        anchor_kernel,
        in_specs=[VM] * 5,
        out_specs=VM,
        out_shape=jax.ShapeDtypeStruct(q.shape, BF16),
        compiler_params=pltpu.CompilerParams(vmem_limit_bytes=24 << 20),
        cost_estimate=pl.CostEstimate(
            flops=4 * rows * 4 * 2 * rows * HDIM, bytes_accessed=3 << 20, transcendentals=4 * rows * 2 * rows
        ),
        name="anchor_block",
    )(near(q), near(kva), near(kvb), near(acc), near(stat))


def paths(size):
    far, near = (2 * size) // 5, size // 5
    hubs = [far, size - far, near, size - near]
    have = {0, *hubs}
    sends = []
    for sign in (1, -1):
        pairs = []
        for h in sorted(have):
            dst = (h + sign) % size
            if dst not in have and all(dst != d for level in sends for _, d in level):
                pairs.append((h, dst))
        sends.append(pairs)
    reached = have | {d for level in sends for _, d in level}
    for d in range(size):
        if d not in reached:
            sends.append([(min([0, *hubs], key=lambda h: abs(h - d)), d)])
    return hubs, sends


def chosen(ctx, places, new, old):
    hit = functools.reduce(jnp.logical_or, [ctx == p for p in places])
    return jnp.where(hit, new, old)


def shards(hidden, query_hidden, norm_gain, w_query, w_key, w_value):
    rows = hidden.shape[0]
    toks = query_hidden.shape[0]
    subs = lax.axis_size("sub")
    ctxs = lax.axis_size("ctx")
    slots = ctxs * subs
    gain = norm_gain[None, :]
    ctx = lax.axis_index("ctx")
    swap = [(i, (i + 1) % subs) for i in range(subs)]

    qsend = first_call(ctxs, slots, rows, query_hidden, gain, w_query)
    queries = lax.all_to_all(qsend, "ctx", 0, 0, tiled=True)
    anchor, normed = anchor_rows_call(slots, hidden, gain, w_key, w_value)
    hubs, sends = paths(ctxs)
    arrived = [lax.ppermute(anchor, "ctx", [(0, h)]) for h in hubs]
    kv, normed, qkv = other_rows_call(
        slots, hidden, query_hidden, gain, w_key, w_value, anchor, normed
    )
    kv_other = lax.ppermute(kv, "sub", swap)
    qkv_other = lax.ppermute(qkv, "sub", swap)
    q = q_call(slots, normed, w_query)
    hub = anchor
    for h, value in zip(hubs, arrived):
        hub = chosen(ctx, [h], value, hub)
    arrived = [lax.ppermute(hub, "ctx", pairs) for pairs in sends]
    for pairs, value in zip(sends, arrived):
        hub = chosen(ctx, [d for _, d in pairs], value, hub)
    hub_other = lax.ppermute(hub, "sub", swap)
    parts = partial_call(toks, queries, kv, kv_other, qkv, qkv_other)
    mine = lax.all_to_all(parts, "ctx", 0, 0, tiled=True)
    mark = mark_call(qkv)
    acc, stat = own_call(q, kv, kv_other)
    context_out = anchor_call(q, hub, hub_other, acc, stat)
    query_out = combine_call(ctxs, toks, mine, mark)
    return (context_out, query_out)


def solution(mesh):
    rows = P(("grp", "ctx", "sub"), None)
    cols = P(None, "head")
    outs = P(("grp", "ctx", "sub"), "head")
    return jax.shard_map(
        shards,
        mesh=mesh,
        in_specs=(rows, rows, P(), cols, cols, cols),
        out_specs=(outs, outs),
        check_vma=False,
    )
```
